128 devices in a mesh: rep: 4 (over x_hi, core), tp: 32 (over z, x_lo, y).
Axes of the slice: x: 4 (x_hi: 2, x_lo: 2; x = x_hi * 2 + x_lo), y: 4, z: 4, core: 2. Of those that a mesh axis runs over, the one named last changes fastest.
Arguments:
- trainer_query: float32 [128, 64, 8192], P(('rep', 'tp')), may hold values from -6 to 6
- trainer_output: float32 [128, 8192, 64], P(('rep', 'tp')), may hold values from -6 to 6
- probes: bfloat16 [768, 8192], replicated, may hold values from -0.0625 to 0.0625
- shard_block: int32 [128], replicated, may hold values from 0 to 127, each once
- slice_owner: int32 [32], replicated, may hold values from 0 to 31, each once
Outputs:
- query_slices: bfloat16 [32, 8192, 256], P('tp')
- output_slices: bfloat16 [32, 256, 8192], P('tp')
- query_prints: float32 [32, 768, 256], P('tp')
- output_prints: float32 [32, 256, 768], P('tp')
The draws below stay inside these ranges and needn't reach their ends.
Inputs may be any that keep to these rules, and one draw needn't show every extreme that they name: `shard_block`: a permutation: each number once. `slice_owner`: a permutation: each number once.
All inputs are finite; a program needn't handle non-finite values.
Results may differ from the reference program's by a relative error of at most 0.0029.
Values may be sent and summed in bfloat16 or wider, within the bound.
No kernel may reach another device: no remote copies, remote signals or barrier semaphores. Data moves between devices by JAX's collectives and lax.ppermute only.
A program may use at most 128 MiB of HBM per device.

```python
import jax
import jax.numpy as jnp

D = 8192
PROBES = 768
HQ = 8192
SHARD = 64
SLICE = 256
N_TP = 32
DEVICES = 128


def shard_levels(rng, extent, shards, low, high):
    loudness = 1.0
    for dim, blocks in shards:
        heights = jax.random.uniform(jax.random.fold_in(jax.random.fold_in(rng, 6), dim), (blocks,), jnp.float32, low / len(shards), high / len(shards))
        loudness = loudness * jnp.repeat(jnp.exp(heights), extent[dim] // blocks).reshape((-1,) + (1,) * (len(extent) - 1 - dim))
    return loudness


def noise(stream_key, shape, deviation, reach, shards=(), kind=jnp.bfloat16):
    entries = deviation * jax.random.normal(stream_key, shape, jnp.float32)
    if shards:
        entries = entries * shard_levels(stream_key, shape, shards, -0.22, 0.18)
    return jnp.clip(entries, -reach, reach).astype(kind)


def setup_inputs(seed: int = 0) -> dict:
    streams_of = jax.random.split(jax.random.key(seed), 6)
    return {
        "trainer_query": noise(streams_of[0], (DEVICES, SHARD, HQ), 1.0, 6.0, ((0, 128),), jnp.float32),
        "trainer_output": noise(streams_of[1], (DEVICES, HQ, SHARD), 1.0, 6.0, ((0, 128),), jnp.float32),
        "probes": noise(streams_of[2], (PROBES, D), D ** -0.5, 0.0625),
        "shard_block": jax.random.permutation(streams_of[3], DEVICES).astype(jnp.int32),
        "slice_owner": jax.random.permutation(streams_of[4], N_TP).astype(jnp.int32),
    }


def reference(trainer_query, trainer_output, probes, shard_block, slice_owner):
    positions = jnp.arange(DEVICES, dtype=jnp.int32)
    inverse = jnp.zeros((DEVICES,), jnp.int32).at[shard_block].set(positions)
    query_full = trainer_query.astype(jnp.bfloat16)[inverse].reshape(D, HQ)
    output_full = jnp.transpose(trainer_output.astype(jnp.bfloat16)[inverse], (1, 0, 2)).reshape(HQ, D)
    query_slices = jnp.transpose(query_full.reshape(D, N_TP, SLICE)[:, slice_owner], (1, 0, 2))
    output_slices = output_full.reshape(N_TP, SLICE, D)[slice_owner]
    probe_wide = probes.astype(jnp.float32)
    query_prints = jnp.einsum("pd,jdc->jpc", probe_wide, query_slices.astype(jnp.float32))
    output_prints = jnp.einsum("jcd,pd->jcp", output_slices.astype(jnp.float32), probe_wide)
    return (query_slices, output_slices, query_prints, output_prints)
```

```python
import jax
import jax.numpy as jnp
from jax import lax
from jax.experimental import pallas as pl
from jax.experimental.pallas import tpu as pltpu
from jax.sharding import PartitionSpec as P


LANES = 128
MIB = 1 << 20


def params(mib):
    return pltpu.CompilerParams(vmem_limit_bytes=mib * MIB)


def in_hbm(x):
    return pltpu.with_memory_space_constraint(x, pltpu.HBM)


def in_vmem(x):
    return pltpu.with_memory_space_constraint(x, pltpu.VMEM)


def invert(dst, perm, count):
    def put(i, carry):
        dst[perm[i]] = i
        return carry

    lax.fori_loop(0, count, put, 0)


def pack_kernel(owner, q_hbm, o_hbm, out, qv, ov, inv, sems):
    x_count, halves, tp_count = out.shape[:3]
    width = halves * LANES
    chunks = sems.shape[1]
    step = qv.shape[1] // chunks

    def copies(c):
        at = (slice(None), pl.ds(c * step, step))
        return (
            pltpu.make_async_copy(q_hbm.at[at], qv.at[at], sems.at[0, c]),
            pltpu.make_async_copy(o_hbm.at[at], ov.at[at], sems.at[1, c]),
        )

    for c in range(chunks):
        for copy in copies(c):
            copy.start()
    invert(inv, owner, tp_count)
    for c in range(chunks):
        for copy in copies(c):
            copy.wait()
        for j in range(c * step // width, (c + 1) * step // width):
            t = inv[j]
            for h in range(halves):
                at = j * width + h * LANES
                q = qv[:, at : at + LANES].astype(jnp.bfloat16)
                o = ov[:, at : at + LANES].astype(jnp.bfloat16)
                for x in range(x_count):
                    out[x, h, t, :, :LANES] = q
                    out[x, h, t, :, LANES:] = o


def dot_kernel(block_of, recv, probes, out, rows, inv):
    count, size, _ = recv.shape
    invert(inv, block_of, count)

    def put(b, carry):
        rows[pl.ds(pl.multiple_of(b * size, size), size), :] = recv[inv[b]]
        return carry

    lax.fori_loop(0, count, put, 0, unroll=4)
    out[...] = jnp.dot(probes[...], rows[...], preferred_element_type=jnp.float32)


def write_half(block_of, half, recv, q_out, o_out, turned, inv, sems):
    count, size, _ = recv.shape
    lanes = pl.ds(pl.multiple_of(half * LANES, LANES), LANES)
    invert(inv, block_of, count)

    def q_copy(s):
        row = pl.multiple_of(block_of[s] * size, size)
        return pltpu.make_async_copy(
            recv.at[s, :, pl.ds(0, LANES)], q_out.at[pl.ds(row, size), lanes], sems.at[0]
        )

    def o_copy(c, step):
        at = pl.ds(c * step, step)
        return pltpu.make_async_copy(turned.at[:, at], o_out.at[lanes, at], sems.at[1])

    def send(s, carry):
        q_copy(s).start()
        return carry

    lax.fori_loop(0, count, send, 0)
    chunks = 8
    step = count * size // chunks
    per = step // LANES
    for c in range(chunks):
        for k in range(per):
            pair = 2 * (c * per + k)
            tile = jnp.concatenate([recv[inv[pair], :, LANES:], recv[inv[pair + 1], :, LANES:]], axis=0)
            turned[:, pl.ds(c * step + k * LANES, LANES)] = tile.T
        o_copy(c, step).start()

    def finish():
        lax.fori_loop(0, count, lambda s, carry: (q_copy(s).wait(), carry)[1], 0)
        for c in range(chunks):
            o_copy(c, step).wait()

    return finish


def first_kernel(block_of, core, recv, q_out, o_out, turned, inv, sems):
    write_half(block_of, core[0], recv, q_out, o_out, turned, inv, sems)()


def second_kernel(
    block_of, core, recv, own, other, q_in, o_in, q_out, o_out, q_prints, o_prints, turned, inv, sems
):
    finish = write_half(block_of, 1 - core[0], recv, q_out, o_out, turned, inv, sems)
    for prints, half in ((own, core[0]), (other, 1 - core[0])):
        lanes = pl.ds(pl.multiple_of(half * LANES, LANES), LANES)
        q_prints[:, lanes] = prints[:, :LANES]
        o_prints[lanes, :] = prints[:, LANES:].T
    finish()


def per_device(trainer_query, trainer_output, probes, shard_block, slice_owner):
    tp_count = lax.axis_size("tp")
    rep_count = lax.axis_size("rep")
    dev_count = tp_count * rep_count
    shard_rows = trainer_query.shape[1]
    features = trainer_query.shape[2]
    model_width = shard_rows * dev_count
    halves = 2
    width = halves * LANES
    probe_count = probes.shape[0]
    bf16, f32 = jnp.bfloat16, jnp.float32
    smem = pl.BlockSpec(memory_space=pltpu.SMEM)
    vmem = pl.BlockSpec(memory_space=pltpu.VMEM)
    hbm = pl.BlockSpec(memory_space=pltpu.HBM)

    packed = pl.pallas_call(
        pack_kernel,
        out_shape=jax.ShapeDtypeStruct((rep_count // halves, halves, tp_count, shard_rows, width), bf16),
        in_specs=[smem, hbm, hbm],
        out_specs=vmem,
        scratch_shapes=[
            pltpu.VMEM((shard_rows, features), f32),
            pltpu.VMEM((shard_rows, features), f32),
            pltpu.SMEM((tp_count,), jnp.int32),
            pltpu.SemaphoreType.DMA((2, 8)),
        ],
        compiler_params=params(12),
        name="pack",
    )(slice_owner, in_hbm(trainer_query[0]), in_hbm(trainer_output[0].T))

    recv = lax.all_to_all(
        packed.reshape(dev_count, shard_rows, width), ("rep", "tp"), split_axis=0, concat_axis=0, tiled=True
    )
    swap = [(r, r ^ 1) for r in range(rep_count)]
    core = (lax.axis_index("rep") % halves).reshape(1)
    other_recv = lax.ppermute(recv, "rep", swap)

    prints = pl.pallas_call(
        dot_kernel,
        out_shape=jax.ShapeDtypeStruct((probe_count, width), f32),
        in_specs=[smem, vmem, vmem],
        out_specs=vmem,
        scratch_shapes=[pltpu.VMEM((model_width, width), bf16), pltpu.SMEM((dev_count,), jnp.int32)],
        compiler_params=params(14),
        name="prints",
    )(shard_block, recv, probes)
    other_prints = lax.ppermute(prints, "rep", swap)

    scratch = [
        pltpu.VMEM((LANES, model_width), bf16),
        pltpu.SMEM((dev_count,), jnp.int32),
        pltpu.SemaphoreType.DMA((2,)),
    ]
    slices = (
        jax.ShapeDtypeStruct((model_width, width), bf16),
        jax.ShapeDtypeStruct((width, model_width), bf16),
    )
    q_slice, o_slice = pl.pallas_call(
        first_kernel,
        out_shape=slices,
        in_specs=[smem, smem, vmem],
        out_specs=(hbm, hbm),
        scratch_shapes=scratch,
        compiler_params=params(12),
        name="own_half",
    )(shard_block, core, recv)
    q_slice, o_slice, q_prints, o_prints = pl.pallas_call(
        second_kernel,
        out_shape=slices
        + (
            jax.ShapeDtypeStruct((probe_count, width), f32),
            jax.ShapeDtypeStruct((width, probe_count), f32),
        ),
        in_specs=[smem, smem, vmem, vmem, vmem, hbm, hbm],
        out_specs=(hbm, hbm, vmem, vmem),
        scratch_shapes=scratch,
        input_output_aliases={5: 0, 6: 1},
        compiler_params=params(12),
        name="other_half",
    )(shard_block, core, other_recv, prints, other_prints, q_slice, o_slice)
    return (q_slice[None], o_slice[None], q_prints[None], o_prints[None])


def solution(mesh):
    placed = (P(("rep", "tp"), None, None), P(("rep", "tp"), None, None), P(), P(), P())
    return jax.shard_map(
        per_device,
        mesh=mesh,
        in_specs=placed,
        out_specs=(
            P("tp", None, None),
            P("tp", None, None),
            P("tp", None, None),
            P("tp", None, None),
        ),
        check_vma=False,
    )
```

```python
import jax
import jax.numpy as jnp
from jax import lax
from jax.experimental import pallas as pl
from jax.experimental.pallas import tpu as pltpu
from jax.sharding import Mesh
from jax.sharding import PartitionSpec as P


AXES = ("xh", "core", "z", "xl", "y")
SIZES = (2, 2, 4, 2, 4)
GROUP = ("y", "xl", "z", "core", "xh")
LANES = 128
MIB = 1 << 20


def params(mib):
    return pltpu.CompilerParams(vmem_limit_bytes=mib * MIB)


def in_hbm(x):
    return pltpu.with_memory_space_constraint(x, pltpu.HBM)


def in_vmem(x):
    return pltpu.with_memory_space_constraint(x, pltpu.VMEM)


def my_core():
    return lax.axis_index("core")


def place(s):
    axes, stride, at = dict(zip(AXES, SIZES)), 1, 0
    digits = {}
    for name, size in reversed(list(zip(AXES, SIZES))):
        digits[name] = s & (size - 1)
        s = s >> (size.bit_length() - 1)
    for name in reversed(GROUP):
        at = at + digits[name] * stride
        stride *= axes[name]
    return at


def invert(dst, perm, count, where=lambda i: i):
    def put(i, carry):
        dst[perm[i]] = where(i)
        return carry

    lax.fori_loop(0, count, put, 0)


def pack_kernel(owner, q_hbm, o_hbm, out, qv, ov, inv, sems):
    x_count, halves, tp_count = 2, 2, owner.shape[0]
    width = halves * LANES
    chunks = sems.shape[1]
    step = qv.shape[1] // chunks

    def copies(c):
        at = (slice(None), pl.ds(c * step, step))
        return (
            pltpu.make_async_copy(q_hbm.at[at], qv.at[at], sems.at[0, c]),
            pltpu.make_async_copy(o_hbm.at[at], ov.at[at], sems.at[1, c]),
        )

    for c in range(chunks):
        for copy in copies(c):
            copy.start()
    invert(inv, owner, tp_count)
    for c in range(chunks):
        for copy in copies(c):
            copy.wait()
        for j in range(c * step // width, (c + 1) * step // width):
            t = inv[j]
            for h in range(halves):
                at = j * width + h * LANES
                q = qv[:, at : at + LANES].astype(jnp.bfloat16)
                o = ov[:, at : at + LANES].astype(jnp.bfloat16)
                for x in range(x_count):
                    p = place((x * halves + h) * tp_count + t)
                    out[p, :, :LANES] = q
                    out[p, :, LANES:] = o


def dot_kernel(block_of, recv, probes, out, rows, inv):
    count, size, _ = recv.shape
    invert(inv, block_of, count, place)

    def put(b, carry):
        rows[pl.ds(pl.multiple_of(b * size, size), size), :] = recv[inv[b]]
        return carry

    lax.fori_loop(0, count, put, 0, unroll=4)
    out[...] = jnp.dot(probes[...], rows[...], preferred_element_type=jnp.float32)


def write_half(block_of, half, recv, q_out, o_out, turned, inv, sems):
    count, size, _ = recv.shape
    lanes = pl.ds(pl.multiple_of(half * LANES, LANES), LANES)
    invert(inv, block_of, count, place)

    def q_copy(s):
        row = pl.multiple_of(block_of[s] * size, size)
        return pltpu.make_async_copy(
            recv.at[place(s), :, pl.ds(0, LANES)], q_out.at[pl.ds(row, size), lanes], sems.at[0]
        )

    def o_copy(c, step):
        at = pl.ds(c * step, step)
        return pltpu.make_async_copy(turned.at[:, at], o_out.at[lanes, at], sems.at[1])

    def send(s, carry):
        q_copy(s).start()
        return carry

    lax.fori_loop(0, count, send, 0)
    chunks = 8
    step = count * size // chunks
    per = step // LANES
    for c in range(chunks):
        for k in range(per):
            pair = 2 * (c * per + k)
            tile = jnp.concatenate([recv[inv[pair], :, LANES:], recv[inv[pair + 1], :, LANES:]], axis=0)
            turned[:, pl.ds(c * step + k * LANES, LANES)] = tile.T
        o_copy(c, step).start()

    def finish():
        lax.fori_loop(0, count, lambda s, carry: (q_copy(s).wait(), carry)[1], 0)
        for c in range(chunks):
            o_copy(c, step).wait()

    return finish


def first_kernel(block_of, recv, q_out, o_out, turned, inv, sems):
    write_half(block_of, my_core(), recv, q_out, o_out, turned, inv, sems)()


def second_kernel(
    block_of, recv, own, other, q_in, o_in, q_out, o_out, q_prints, o_prints, turned, inv, sems
):
    core = my_core()
    finish = write_half(block_of, 1 - core, recv, q_out, o_out, turned, inv, sems)
    for prints, half in ((own, core), (other, 1 - core)):
        lanes = pl.ds(pl.multiple_of(half * LANES, LANES), LANES)
        q_prints[:, lanes] = prints[:, :LANES]
        o_prints[lanes, :] = prints[:, LANES:].T
    finish()


def per_device(trainer_query, trainer_output, probes, shard_block, slice_owner):
    tp_count = slice_owner.shape[0]
    dev_count = shard_block.shape[0]
    shard_rows = trainer_query.shape[1]
    features = trainer_query.shape[2]
    model_width = shard_rows * dev_count
    halves = 2
    width = halves * LANES
    probe_count = probes.shape[0]
    bf16, f32 = jnp.bfloat16, jnp.float32
    smem = pl.BlockSpec(memory_space=pltpu.SMEM)
    vmem = pl.BlockSpec(memory_space=pltpu.VMEM)
    hbm = pl.BlockSpec(memory_space=pltpu.HBM)

    packed = pl.pallas_call(
        pack_kernel,
        out_shape=jax.ShapeDtypeStruct((dev_count, shard_rows, width), bf16),
        in_specs=[smem, hbm, hbm],
        out_specs=vmem,
        scratch_shapes=[
            pltpu.VMEM((shard_rows, features), f32),
            pltpu.VMEM((shard_rows, features), f32),
            pltpu.SMEM((tp_count,), jnp.int32),
            pltpu.SemaphoreType.DMA((2, 8)),
        ],
        compiler_params=params(12),
        name="pack",
    )(slice_owner, in_hbm(trainer_query[0]), in_hbm(trainer_output[0].T))

    recv = lax.all_to_all(packed, GROUP, split_axis=0, concat_axis=0, tiled=True)
    swap = [(0, 1), (1, 0)]
    other_recv = lax.ppermute(recv, "core", swap)

    prints = pl.pallas_call(
        dot_kernel,
        out_shape=jax.ShapeDtypeStruct((probe_count, width), f32),
        in_specs=[smem, vmem, vmem],
        out_specs=vmem,
        scratch_shapes=[pltpu.VMEM((model_width, width), bf16), pltpu.SMEM((dev_count,), jnp.int32)],
        compiler_params=params(14),
        name="prints",
    )(shard_block, recv, probes)
    other_prints = lax.ppermute(prints, "core", swap)

    scratch = [
        pltpu.VMEM((LANES, model_width), bf16),
        pltpu.SMEM((dev_count,), jnp.int32),
        pltpu.SemaphoreType.DMA((2,)),
    ]
    slices = (
        jax.ShapeDtypeStruct((model_width, width), bf16),
        jax.ShapeDtypeStruct((width, model_width), bf16),
    )
    q_slice, o_slice = pl.pallas_call(
        first_kernel,
        out_shape=slices,
        in_specs=[smem, vmem],
        out_specs=(hbm, hbm),
        scratch_shapes=scratch,
        compiler_params=params(12),
        name="own_half",
    )(shard_block, recv)
    q_slice, o_slice, q_prints, o_prints = pl.pallas_call(
        second_kernel,
        out_shape=slices
        + (
            jax.ShapeDtypeStruct((probe_count, width), f32),
            jax.ShapeDtypeStruct((width, probe_count), f32),
        ),
        in_specs=[smem, vmem, vmem, vmem, hbm, hbm],
        out_specs=(hbm, hbm, vmem, vmem),
        scratch_shapes=scratch,
        input_output_aliases={4: 0, 5: 1},
        compiler_params=params(12),
        name="other_half",
    )(shard_block, other_recv, prints, other_prints, q_slice, o_slice)
    return (q_slice[None], o_slice[None], q_prints[None], o_prints[None])


def solution(mesh):
    fine = Mesh(mesh.devices.reshape(SIZES), AXES)
    placed = (P(AXES, None, None), P(AXES, None, None), P(), P(), P())
    out = P(("z", "xl", "y"), None, None)
    return jax.shard_map(per_device, mesh=fine, in_specs=placed, out_specs=(out, out, out, out), check_vma=False)
```

```python
import jax
import jax.numpy as jnp
from jax import lax
from jax.experimental import pallas as pl
from jax.experimental.pallas import tpu as pltpu
from jax.sharding import Mesh
from jax.sharding import PartitionSpec as P


AXES = ("xh", "core", "z", "xl", "y")
SIZES = (2, 2, 4, 2, 4)
GROUP = ("y", "z", "xh", "xl", "core")
LANES = 128
MIB = 1 << 20


def params(mib):
    return pltpu.CompilerParams(vmem_limit_bytes=mib * MIB)


def in_hbm(x):
    return pltpu.with_memory_space_constraint(x, pltpu.HBM)


def in_vmem(x):
    return pltpu.with_memory_space_constraint(x, pltpu.VMEM)


def my_core():
    return lax.axis_index("core")


def place(s):
    axes, stride, at = dict(zip(AXES, SIZES)), 1, 0
    digits = {}
    for name, size in reversed(list(zip(AXES, SIZES))):
        digits[name] = s & (size - 1)
        s = s >> (size.bit_length() - 1)
    for name in reversed(GROUP):
        at = at + digits[name] * stride
        stride *= axes[name]
    return at


def pack_kernel(owner_hbm, q_hbm, o_hbm, out, owner, qv, ov, inv, sems, owner_sem):
    x_count, halves, tp_count = 2, 2, owner.shape[0]
    width = halves * LANES
    chunks = sems.shape[1]
    step = qv.shape[1] // chunks

    def copies(c):
        at = (slice(None), pl.ds(c * step, step))
        return (
            pltpu.make_async_copy(q_hbm.at[at], qv.at[at], sems.at[0, c]),
            pltpu.make_async_copy(o_hbm.at[at], ov.at[at], sems.at[1, c]),
        )

    owners = pltpu.make_async_copy(owner_hbm, owner, owner_sem)
    owners.start()
    for c in range(chunks):
        for copy in copies(c):
            copy.start()
    owners.wait()
    for t in range(tp_count):
        inv[owner[t]] = t
    for c in range(chunks):
        for copy in copies(c):
            copy.wait()
        for j in range(c * step // width, (c + 1) * step // width):
            t = inv[j]
            for h in range(halves):
                at = j * width + h * LANES
                q = qv[:, at : at + LANES].astype(jnp.bfloat16)
                o = ov[:, at : at + LANES].astype(jnp.bfloat16)
                for x in range(x_count):
                    p = place((x * halves + h) * tp_count + t)
                    out[p, :, :LANES] = q
                    out[p, :, LANES:] = o


def dot_kernel(block_of, recv, probes, out, rows, inv):
    count, size, _ = recv.shape
    for s in range(count):
        inv[block_of[s]] = place(s)
    parts = 4
    per = count // parts
    for c in range(parts):
        for b in range(c * per, (c + 1) * per):
            rows[b * size : (b + 1) * size, :] = recv[inv[b]]
        at = slice(c * per * size, (c + 1) * per * size)
        part = jnp.dot(probes[:, at], rows[at, :], preferred_element_type=jnp.float32)
        out[...] = part if c == 0 else out[...] + part


def write_half(block_of, half, recv, q_out, o_out, turned, inv, sems):
    count, size, _ = recv.shape
    lanes = pl.ds(pl.multiple_of(half * LANES, LANES), LANES)
    for s in range(count):
        inv[block_of[s]] = place(s)
        row = pl.multiple_of(block_of[s] * size, size)
        pltpu.make_async_copy(
            recv.at[place(s), :, pl.ds(0, LANES)], q_out.at[pl.ds(row, size), lanes], sems.at[0]
        ).start()
    chunks = 8
    step = count * size // chunks
    per = step // LANES
    for c in range(chunks):
        for k in range(per):
            pair = 2 * (c * per + k)
            tile = jnp.concatenate([recv[inv[pair], :, LANES:], recv[inv[pair + 1], :, LANES:]], axis=0)
            turned[:, pl.ds(c * step + k * LANES, LANES)] = tile.T
        at = pl.ds(c * step, step)
        pltpu.make_async_copy(turned.at[:, at], o_out.at[lanes, at], sems.at[1]).start()

    def finish():
        pltpu.make_async_copy(q_out.at[:, lanes], q_out.at[:, lanes], sems.at[0]).wait()
        pltpu.make_async_copy(turned, o_out.at[lanes, :], sems.at[1]).wait()

    return finish


def first_kernel(block_of, recv, q_out, o_out, turned, inv, sems):
    write_half(block_of, my_core(), recv, q_out, o_out, turned, inv, sems)()


def second_kernel(
    block_of, recv, own, other, q_in, o_in, q_out, o_out, q_prints, o_prints, turned, inv, sems
):
    core = my_core()
    finish = write_half(block_of, 1 - core, recv, q_out, o_out, turned, inv, sems)
    for prints, half in ((own, core), (other, 1 - core)):
        lanes = pl.ds(pl.multiple_of(half * LANES, LANES), LANES)
        q_prints[:, lanes] = prints[:, :LANES]
        o_prints[lanes, :] = prints[:, LANES:].T
    finish()


def per_device(trainer_query, trainer_output, probes, shard_block, slice_owner):
    tp_count = slice_owner.shape[0]
    dev_count = shard_block.shape[0]
    shard_rows = trainer_query.shape[1]
    features = trainer_query.shape[2]
    model_width = shard_rows * dev_count
    halves = 2
    width = halves * LANES
    probe_count = probes.shape[0]
    bf16, f32 = jnp.bfloat16, jnp.float32
    smem = pl.BlockSpec(memory_space=pltpu.SMEM)
    vmem = pl.BlockSpec(memory_space=pltpu.VMEM)
    hbm = pl.BlockSpec(memory_space=pltpu.HBM)

    packed = pl.pallas_call(
        pack_kernel,
        out_shape=jax.ShapeDtypeStruct((dev_count, shard_rows, width), bf16),
        in_specs=[hbm, hbm, hbm],
        out_specs=vmem,
        scratch_shapes=[
            pltpu.SMEM((tp_count,), jnp.int32),
            pltpu.VMEM((shard_rows, features), f32),
            pltpu.VMEM((shard_rows, features), f32),
            pltpu.SMEM((tp_count,), jnp.int32),
            pltpu.SemaphoreType.DMA((2, 8)),
            pltpu.SemaphoreType.DMA(()),
        ],
        compiler_params=params(12),
        name="pack",
    )(in_hbm(slice_owner), in_hbm(trainer_query[0]), in_hbm(trainer_output[0].T))

    recv = lax.all_to_all(packed, GROUP, split_axis=0, concat_axis=0, tiled=True)
    swap = [(0, 1), (1, 0)]
    other_recv = lax.ppermute(recv, "core", swap)

    prints = pl.pallas_call(
        dot_kernel,
        out_shape=jax.ShapeDtypeStruct((probe_count, width), f32),
        in_specs=[smem, vmem, vmem],
        out_specs=vmem,
        scratch_shapes=[pltpu.VMEM((model_width, width), bf16), pltpu.SMEM((dev_count,), jnp.int32)],
        compiler_params=params(14),
        name="prints",
    )(shard_block, recv, probes)
    other_prints = lax.ppermute(prints, "core", swap)

    scratch = [
        pltpu.VMEM((LANES, model_width), bf16),
        pltpu.SMEM((dev_count,), jnp.int32),
        pltpu.SemaphoreType.DMA((2,)),
    ]
    slices = (
        jax.ShapeDtypeStruct((model_width, width), bf16),
        jax.ShapeDtypeStruct((width, model_width), bf16),
    )
    q_slice, o_slice = pl.pallas_call(
        first_kernel,
        out_shape=slices,
        in_specs=[smem, vmem],
        out_specs=(hbm, hbm),
        scratch_shapes=scratch,
        compiler_params=params(12),
        name="own_half",
    )(shard_block, recv)
    q_slice, o_slice, q_prints, o_prints = pl.pallas_call(
        second_kernel,
        out_shape=slices
        + (
            jax.ShapeDtypeStruct((probe_count, width), f32),
            jax.ShapeDtypeStruct((width, probe_count), f32),
        ),
        in_specs=[smem, vmem, vmem, vmem, hbm, hbm],
        out_specs=(hbm, hbm, vmem, vmem),
        scratch_shapes=scratch,
        input_output_aliases={4: 0, 5: 1},
        compiler_params=params(12),
        name="other_half",
    )(shard_block, other_recv, prints, other_prints, q_slice, o_slice)
    return (q_slice[None], o_slice[None], q_prints[None], o_prints[None])


def solution(mesh):
    fine = Mesh(mesh.devices.reshape(SIZES), AXES)
    placed = (P(AXES, None, None), P(AXES, None, None), P(), P(), P())
    out = P(("z", "xl", "y"), None, None)
    return jax.shard_map(per_device, mesh=fine, in_specs=placed, out_specs=(out, out, out, out), check_vma=False)
```

```python
import jax
import jax.numpy as jnp
from jax import lax
from jax.experimental import pallas as pl
from jax.experimental.pallas import tpu as pltpu
from jax.sharding import Mesh
from jax.sharding import PartitionSpec as P


AXES = ("xh", "core", "z", "xl", "y")
SIZES = (2, 2, 4, 2, 4)
GROUP = ("y", "z", "xh", "xl", "core")
LANES = 128
MIB = 1 << 20


def params(mib):
    return pltpu.CompilerParams(vmem_limit_bytes=mib * MIB)


def in_hbm(x):
    return pltpu.with_memory_space_constraint(x, pltpu.HBM)


def in_vmem(x):
    return pltpu.with_memory_space_constraint(x, pltpu.VMEM)


def my_core():
    return lax.axis_index("core")


def place(s):
    axes, stride, at = dict(zip(AXES, SIZES)), 1, 0
    digits = {}
    for name, size in reversed(list(zip(AXES, SIZES))):
        digits[name] = s & (size - 1)
        s = s >> (size.bit_length() - 1)
    for name in reversed(GROUP):
        at = at + digits[name] * stride
        stride *= axes[name]
    return at


def pack_kernel(owner_hbm, q_hbm, o_hbm, out, owner, qv, ov, inv, sems, owner_sem):
    x_count, halves, tp_count = 2, 2, owner.shape[0]
    width = halves * LANES
    chunks = sems.shape[1]
    step = qv.shape[1] // chunks

    def copies(c):
        at = (slice(None), pl.ds(c * step, step))
        return (
            pltpu.make_async_copy(q_hbm.at[at], qv.at[at], sems.at[0, c]),
            pltpu.make_async_copy(o_hbm.at[at], ov.at[at], sems.at[1, c]),
        )

    owners = pltpu.make_async_copy(owner_hbm, owner, owner_sem)
    owners.start()
    for c in range(chunks):
        for copy in copies(c):
            copy.start()
    owners.wait()
    for t in range(tp_count):
        inv[owner[t]] = t
    for c in range(chunks):
        for copy in copies(c):
            copy.wait()
        for j in range(c * step // width, (c + 1) * step // width):
            t = inv[j]
            for h in range(halves):
                at = j * width + h * LANES
                q = qv[:, at : at + LANES].astype(jnp.bfloat16)
                o = ov[:, at : at + LANES].astype(jnp.bfloat16)
                for x in range(x_count):
                    p = place((x * halves + h) * tp_count + t)
                    out[p, :, :LANES] = q
                    out[p, :, LANES:] = o


def dot_kernel(block_of, recv, probes, out, rows, inv):
    count, size, _ = recv.shape
    for s in range(count):
        inv[block_of[s]] = place(s)
    parts = 4
    per = count // parts
    for c in range(parts):
        for b in range(c * per, (c + 1) * per):
            rows[b * size : (b + 1) * size, :] = recv[inv[b]]
        at = slice(c * per * size, (c + 1) * per * size)
        part = jnp.dot(probes[:, at], rows[at, :], preferred_element_type=jnp.float32)
        out[...] = part if c == 0 else out[...] + part


def write_half(half, block_hbm, recv, prints, outs, blocks, turned, prints_turned, inv, sems):
    q_out, o_out, q_prints, o_prints = outs
    count, size, _ = recv.shape
    lanes = pl.ds(pl.multiple_of(half * LANES, LANES), LANES)
    table = pltpu.make_async_copy(block_hbm, blocks, sems.at[4])
    q_prints_copy = pltpu.make_async_copy(prints.at[:, pl.ds(0, LANES)], q_prints.at[:, lanes], sems.at[2])
    o_prints_copy = pltpu.make_async_copy(prints_turned, o_prints.at[lanes, :], sems.at[3])
    table.start()
    q_prints_copy.start()
    prints_turned[...] = prints[:, LANES:].T
    o_prints_copy.start()
    table.wait()
    for s in range(count):
        inv[blocks[s]] = place(s)
        row = pl.multiple_of(blocks[s] * size, size)
        pltpu.make_async_copy(
            recv.at[place(s), :, pl.ds(0, LANES)], q_out.at[pl.ds(row, size), lanes], sems.at[0]
        ).start()
    chunks = 8
    step = count * size // chunks
    per = step // LANES
    for c in range(chunks):
        for k in range(per):
            pair = 2 * (c * per + k)
            tile = jnp.concatenate([recv[inv[pair], :, LANES:], recv[inv[pair + 1], :, LANES:]], axis=0)
            turned[:, pl.ds(c * step + k * LANES, LANES)] = tile.T
        at = pl.ds(c * step, step)
        pltpu.make_async_copy(turned.at[:, at], o_out.at[lanes, at], sems.at[1]).start()
    q_prints_copy.wait()
    o_prints_copy.wait()
    pltpu.make_async_copy(q_out.at[:, lanes], q_out.at[:, lanes], sems.at[0]).wait()
    pltpu.make_async_copy(turned, o_out.at[lanes, :], sems.at[1]).wait()


def own_kernel(block_hbm, recv, prints, *rest):
    write_half(my_core(), block_hbm, recv, prints, rest[:4], *rest[4:])


def other_kernel(block_hbm, recv, prints, *rest):
    write_half(1 - my_core(), block_hbm, recv, prints, rest[4:8], *rest[8:])


def per_device(trainer_query, trainer_output, probes, shard_block, slice_owner):
    tp_count = slice_owner.shape[0]
    dev_count = shard_block.shape[0]
    shard_rows = trainer_query.shape[1]
    features = trainer_query.shape[2]
    model_width = shard_rows * dev_count
    halves = 2
    width = halves * LANES
    probe_count = probes.shape[0]
    bf16, f32 = jnp.bfloat16, jnp.float32
    smem = pl.BlockSpec(memory_space=pltpu.SMEM)
    vmem = pl.BlockSpec(memory_space=pltpu.VMEM)
    hbm = pl.BlockSpec(memory_space=pltpu.HBM)

    packed = pl.pallas_call(
        pack_kernel,
        out_shape=jax.ShapeDtypeStruct((dev_count, shard_rows, width), bf16),
        in_specs=[hbm, hbm, hbm],
        out_specs=vmem,
        scratch_shapes=[
            pltpu.SMEM((tp_count,), jnp.int32),
            pltpu.VMEM((shard_rows, features), f32),
            pltpu.VMEM((shard_rows, features), f32),
            pltpu.SMEM((tp_count,), jnp.int32),
            pltpu.SemaphoreType.DMA((2, 8)),
            pltpu.SemaphoreType.DMA(()),
        ],
        compiler_params=params(12),
        name="pack",
    )(in_hbm(slice_owner), in_hbm(trainer_query[0]), in_hbm(trainer_output[0].T))

    recv = lax.all_to_all(packed, GROUP, split_axis=0, concat_axis=0, tiled=True)
    swap = [(0, 1), (1, 0)]
    other_recv = lax.ppermute(recv, "core", swap)

    prints = pl.pallas_call(
        dot_kernel,
        out_shape=jax.ShapeDtypeStruct((probe_count, width), f32),
        in_specs=[smem, vmem, vmem],
        out_specs=vmem,
        scratch_shapes=[pltpu.VMEM((model_width, width), bf16), pltpu.SMEM((dev_count,), jnp.int32)],
        compiler_params=params(14),
        name="prints",
    )(shard_block, recv, probes)
    other_prints = lax.ppermute(prints, "core", swap)

    half = dict(
        out_shape=(
            jax.ShapeDtypeStruct((model_width, width), bf16),
            jax.ShapeDtypeStruct((width, model_width), bf16),
            jax.ShapeDtypeStruct((probe_count, width), f32),
            jax.ShapeDtypeStruct((width, probe_count), f32),
        ),
        out_specs=(hbm,) * 4,
        scratch_shapes=[
            pltpu.SMEM((dev_count,), jnp.int32),
            pltpu.VMEM((LANES, model_width), bf16),
            pltpu.VMEM((LANES, probe_count), f32),
            pltpu.SMEM((dev_count,), jnp.int32),
            pltpu.SemaphoreType.DMA((5,)),
        ],
        compiler_params=params(12),
    )
    outs = pl.pallas_call(own_kernel, in_specs=[vmem] * 3, name="own_half", **half)(shard_block, recv, prints)
    outs = pl.pallas_call(
        other_kernel,
        in_specs=[vmem] * 3 + [hbm] * 4,
        input_output_aliases={3: 0, 4: 1, 5: 2, 6: 3},
        name="other_half",
        **half,
    )(shard_block, other_recv, other_prints, *outs)
    return tuple(out[None] for out in outs)


def solution(mesh):
    fine = Mesh(mesh.devices.reshape(SIZES), AXES)
    placed = (P(AXES, None, None), P(AXES, None, None), P(), P(), P())
    out = P(("z", "xl", "y"), None, None)
    return jax.shard_map(per_device, mesh=fine, in_specs=placed, out_specs=(out, out, out, out), check_vma=False)
```

```python
import jax
import jax.numpy as jnp
from jax import lax
from jax.experimental import pallas as pl
from jax.experimental.pallas import tpu as pltpu
from jax.sharding import Mesh
from jax.sharding import PartitionSpec as P


AXES = ("xh", "core", "z", "xl", "y")
SIZES = (2, 2, 4, 2, 4)
GROUP = ("y", "z", "xh", "xl", "core")
LANES = 128
MIB = 1 << 20


def params(mib):
    return pltpu.CompilerParams(vmem_limit_bytes=mib * MIB)


def in_hbm(x):
    return pltpu.with_memory_space_constraint(x, pltpu.HBM)


def in_vmem(x):
    return pltpu.with_memory_space_constraint(x, pltpu.VMEM)


def my_core():
    return lax.axis_index("core")


def place(s):
    axes, stride, at = dict(zip(AXES, SIZES)), 1, 0
    digits = {}
    for name, size in reversed(list(zip(AXES, SIZES))):
        digits[name] = s & (size - 1)
        s = s >> (size.bit_length() - 1)
    for name in reversed(GROUP):
        at = at + digits[name] * stride
        stride *= axes[name]
    return at


def pack_kernel(owner_hbm, q_hbm, o_hbm, out, owner, qv, ov, inv, sems, owner_sem):
    x_count, halves, tp_count = 2, 2, owner.shape[0]
    width = halves * LANES
    chunks = sems.shape[1]
    step = qv.shape[1] // chunks

    def copies(c):
        at = (slice(None), pl.ds(c * step, step))
        return (
            pltpu.make_async_copy(q_hbm.at[at], qv.at[at], sems.at[0, c]),
            pltpu.make_async_copy(o_hbm.at[at], ov.at[at], sems.at[1, c]),
        )

    owners = pltpu.make_async_copy(owner_hbm, owner, owner_sem)
    owners.start()
    for c in range(chunks):
        for copy in copies(c):
            copy.start()
    owners.wait()
    for t in range(tp_count):
        inv[owner[t]] = t
    for c in range(chunks):
        for copy in copies(c):
            copy.wait()
        for j in range(c * step // width, (c + 1) * step // width):
            t = inv[j]
            for h in range(halves):
                at = j * width + h * LANES
                q = qv[:, at : at + LANES].astype(jnp.bfloat16)
                o = ov[:, at : at + LANES].astype(jnp.bfloat16)
                for x in range(x_count):
                    p = place((x * halves + h) * tp_count + t)
                    out[p, :, :LANES] = q
                    out[p, :, LANES:] = o


def dot_kernel(block_of, recv, probes, out, sent, rows, inv):
    count, size, _ = recv.shape
    for s in range(count):
        inv[block_of[s]] = place(s)
    parts = 4
    per = count // parts
    for c in range(parts):
        for b in range(c * per, (c + 1) * per):
            rows[b * size : (b + 1) * size, :] = recv[inv[b]]
        at = slice(c * per * size, (c + 1) * per * size)
        part = jnp.dot(probes[:, at], rows[at, :], preferred_element_type=jnp.float32)
        out[...] = part if c == 0 else out[...] + part
    sent[...] = out[...].astype(sent.dtype)


def write_half(half, block_hbm, recv, prints, outs, blocks, turned, prints_wide, prints_turned, inv, sems):
    q_out, o_out, q_prints, o_prints = outs
    count, size, _ = recv.shape
    lanes = pl.ds(pl.multiple_of(half * LANES, LANES), LANES)
    table = pltpu.make_async_copy(block_hbm, blocks, sems.at[4])
    q_prints_copy = pltpu.make_async_copy(prints_wide, q_prints.at[:, lanes], sems.at[2])
    o_prints_copy = pltpu.make_async_copy(prints_turned, o_prints.at[lanes, :], sems.at[3])
    table.start()
    prints_wide[...] = prints[:, :LANES].astype(jnp.float32)
    q_prints_copy.start()
    prints_turned[...] = prints[:, LANES:].astype(jnp.float32).T
    o_prints_copy.start()
    table.wait()
    for s in range(count):
        inv[blocks[s]] = place(s)
    chunks = 8
    step = count * size // chunks
    per = step // LANES

    def q_copy(s):
        row = pl.multiple_of(blocks[s] * size, size)
        return pltpu.make_async_copy(
            recv.at[place(s), :, pl.ds(0, LANES)], q_out.at[pl.ds(row, size), lanes], sems.at[0]
        )

    for c in range(chunks):
        for k in range(per):
            pair = 2 * (c * per + k)
            q_copy(pair).start()
            q_copy(pair + 1).start()
            tile = jnp.concatenate([recv[inv[pair], :, LANES:], recv[inv[pair + 1], :, LANES:]], axis=0)
            turned[:, pl.ds(c * step + k * LANES, LANES)] = tile.T
        at = pl.ds(c * step, step)
        pltpu.make_async_copy(turned.at[:, at], o_out.at[lanes, at], sems.at[1]).start()
    q_prints_copy.wait()
    o_prints_copy.wait()
    pltpu.make_async_copy(q_out.at[:, lanes], q_out.at[:, lanes], sems.at[0]).wait()
    pltpu.make_async_copy(turned, o_out.at[lanes, :], sems.at[1]).wait()


def own_kernel(block_hbm, recv, prints, *rest):
    write_half(my_core(), block_hbm, recv, prints, rest[:4], *rest[4:])


def other_kernel(block_hbm, recv, prints, *rest):
    write_half(1 - my_core(), block_hbm, recv, prints, rest[4:8], *rest[8:])


def per_device(trainer_query, trainer_output, probes, shard_block, slice_owner):
    tp_count = slice_owner.shape[0]
    dev_count = shard_block.shape[0]
    shard_rows = trainer_query.shape[1]
    features = trainer_query.shape[2]
    model_width = shard_rows * dev_count
    halves = 2
    width = halves * LANES
    probe_count = probes.shape[0]
    bf16, f32 = jnp.bfloat16, jnp.float32
    smem = pl.BlockSpec(memory_space=pltpu.SMEM)
    vmem = pl.BlockSpec(memory_space=pltpu.VMEM)
    hbm = pl.BlockSpec(memory_space=pltpu.HBM)

    packed = pl.pallas_call(
        pack_kernel,
        out_shape=jax.ShapeDtypeStruct((dev_count, shard_rows, width), bf16),
        in_specs=[hbm, hbm, hbm],
        out_specs=vmem,
        scratch_shapes=[
            pltpu.SMEM((tp_count,), jnp.int32),
            pltpu.VMEM((shard_rows, features), f32),
            pltpu.VMEM((shard_rows, features), f32),
            pltpu.SMEM((tp_count,), jnp.int32),
            pltpu.SemaphoreType.DMA((2, 8)),
            pltpu.SemaphoreType.DMA(()),
        ],
        compiler_params=params(12),
        name="pack",
    )(in_hbm(slice_owner), in_hbm(trainer_query[0]), in_hbm(trainer_output[0].T))

    recv = lax.all_to_all(packed, GROUP, split_axis=0, concat_axis=0, tiled=True)
    swap = [(0, 1), (1, 0)]
    other_recv = lax.ppermute(recv, "core", swap)

    prints, sent = pl.pallas_call(
        dot_kernel,
        out_shape=(
            jax.ShapeDtypeStruct((probe_count, width), f32),
            jax.ShapeDtypeStruct((probe_count, width), bf16),
        ),
        in_specs=[smem, vmem, vmem],
        out_specs=(vmem, vmem),
        scratch_shapes=[pltpu.VMEM((model_width, width), bf16), pltpu.SMEM((dev_count,), jnp.int32)],
        compiler_params=params(14),
        name="prints",
    )(shard_block, recv, probes)
    other_prints = lax.ppermute(sent, "core", swap)

    half = dict(
        out_shape=(
            jax.ShapeDtypeStruct((model_width, width), bf16),
            jax.ShapeDtypeStruct((width, model_width), bf16),
            jax.ShapeDtypeStruct((probe_count, width), f32),
            jax.ShapeDtypeStruct((width, probe_count), f32),
        ),
        out_specs=(hbm,) * 4,
        scratch_shapes=[
            pltpu.SMEM((dev_count,), jnp.int32),
            pltpu.VMEM((LANES, model_width), bf16),
            pltpu.VMEM((probe_count, LANES), f32),
            pltpu.VMEM((LANES, probe_count), f32),
            pltpu.SMEM((dev_count,), jnp.int32),
            pltpu.SemaphoreType.DMA((5,)),
        ],
        compiler_params=params(12),
    )
    outs = pl.pallas_call(own_kernel, in_specs=[vmem] * 3, name="own_half", **half)(shard_block, recv, prints)
    outs = pl.pallas_call(
        other_kernel,
        in_specs=[vmem] * 3 + [hbm] * 4,
        input_output_aliases={3: 0, 4: 1, 5: 2, 6: 3},
        name="other_half",
        **half,
    )(shard_block, other_recv, other_prints, *outs)
    return tuple(out[None] for out in outs)


def solution(mesh):
    fine = Mesh(mesh.devices.reshape(SIZES), AXES)
    placed = (P(AXES, None, None), P(AXES, None, None), P(), P(), P())
    out = P(("z", "xl", "y"), None, None)
    return jax.shard_map(per_device, mesh=fine, in_specs=placed, out_specs=(out, out, out, out), check_vma=False)
```

```python
import jax
import jax.numpy as jnp
from jax import lax
from jax.experimental import pallas as pl
from jax.experimental.pallas import tpu as pltpu
from jax.sharding import Mesh
from jax.sharding import PartitionSpec as P


AXES = ("xh", "core", "z", "xl", "y")
SIZES = (2, 2, 4, 2, 4)
GROUP = ("y", "core", "xl", "z", "xh")
LANES = 128
MIB = 1 << 20


def params(mib):
    return pltpu.CompilerParams(vmem_limit_bytes=mib * MIB)


def in_hbm(x):
    return pltpu.with_memory_space_constraint(x, pltpu.HBM)


def in_vmem(x):
    return pltpu.with_memory_space_constraint(x, pltpu.VMEM)


def my_core():
    return lax.axis_index("core")


def place(s):
    axes, stride, at = dict(zip(AXES, SIZES)), 1, 0
    digits = {}
    for name, size in reversed(list(zip(AXES, SIZES))):
        digits[name] = s & (size - 1)
        s = s >> (size.bit_length() - 1)
    for name in reversed(GROUP):
        at = at + digits[name] * stride
        stride *= axes[name]
    return at


def pack_kernel(owner_hbm, q_hbm, o_hbm, out, owner, qv, ov, inv, sems, owner_sem):
    x_count, halves, tp_count = 2, 2, owner.shape[0]
    width = halves * LANES
    chunks = sems.shape[1]
    step = qv.shape[1] // chunks

    def copies(c):
        at = (slice(None), pl.ds(c * step, step))
        return (
            pltpu.make_async_copy(q_hbm.at[at], qv.at[at], sems.at[0, c]),
            pltpu.make_async_copy(o_hbm.at[at], ov.at[at], sems.at[1, c]),
        )

    owners = pltpu.make_async_copy(owner_hbm, owner, owner_sem)
    owners.start()
    for c in range(chunks):
        for copy in copies(c):
            copy.start()
    owners.wait()
    for t in range(tp_count):
        inv[owner[t]] = t
    for c in range(chunks):
        for copy in copies(c):
            copy.wait()
        for j in range(c * step // width, (c + 1) * step // width):
            t = inv[j]
            for h in range(halves):
                at = j * width + h * LANES
                q = qv[:, at : at + LANES].astype(jnp.bfloat16)
                o = ov[:, at : at + LANES].astype(jnp.bfloat16)
                for x in range(x_count):
                    p = place((x * halves + h) * tp_count + t)
                    out[p, :, :LANES] = q
                    out[p, :, LANES:] = o


def dot_kernel(block_of, recv, probes, out, sent, rows, inv):
    count, size, _ = recv.shape
    for s in range(count):
        inv[block_of[s]] = place(s)
    parts = 4
    per = count // parts
    for c in range(parts):
        for b in range(c * per, (c + 1) * per):
            rows[b * size : (b + 1) * size, :] = recv[inv[b]]
        at = slice(c * per * size, (c + 1) * per * size)
        part = jnp.dot(probes[:, at], rows[at, :], preferred_element_type=jnp.float32)
        out[...] = part if c == 0 else out[...] + part
    sent[...] = out[...].astype(sent.dtype)


def write_half(half, block_hbm, recv, prints, outs, blocks, turned, prints_wide, prints_turned, inv, sems):
    q_out, o_out, q_prints, o_prints = outs
    count, size, _ = recv.shape
    lanes = pl.ds(pl.multiple_of(half * LANES, LANES), LANES)
    table = pltpu.make_async_copy(block_hbm, blocks, sems.at[4])
    q_prints_copy = pltpu.make_async_copy(prints_wide, q_prints.at[:, lanes], sems.at[2])
    o_prints_copy = pltpu.make_async_copy(prints_turned, o_prints.at[lanes, :], sems.at[3])
    table.start()
    prints_wide[...] = prints[:, :LANES].astype(jnp.float32)
    q_prints_copy.start()
    prints_turned[...] = prints[:, LANES:].astype(jnp.float32).T
    o_prints_copy.start()
    table.wait()
    for s in range(count):
        inv[blocks[s]] = place(s)
    chunks = 8
    step = count * size // chunks
    per = step // LANES

    def q_copy(s):
        row = pl.multiple_of(blocks[s] * size, size)
        return pltpu.make_async_copy(
            recv.at[place(s), :, pl.ds(0, LANES)], q_out.at[pl.ds(row, size), lanes], sems.at[0]
        )

    for c in range(chunks):
        for k in range(per):
            pair = 2 * (c * per + k)
            q_copy(pair).start()
            q_copy(pair + 1).start()
            tile = jnp.concatenate([recv[inv[pair], :, LANES:], recv[inv[pair + 1], :, LANES:]], axis=0)
            turned[:, pl.ds(c * step + k * LANES, LANES)] = tile.T
        at = pl.ds(c * step, step)
        pltpu.make_async_copy(turned.at[:, at], o_out.at[lanes, at], sems.at[1]).start()
    q_prints_copy.wait()
    o_prints_copy.wait()
    pltpu.make_async_copy(q_out.at[:, lanes], q_out.at[:, lanes], sems.at[0]).wait()
    pltpu.make_async_copy(turned, o_out.at[lanes, :], sems.at[1]).wait()


def own_kernel(block_hbm, recv, prints, *rest):
    write_half(my_core(), block_hbm, recv, prints, rest[:4], *rest[4:])


def other_kernel(block_hbm, recv, prints, *rest):
    write_half(1 - my_core(), block_hbm, recv, prints, rest[4:8], *rest[8:])


def per_device(trainer_query, trainer_output, probes, shard_block, slice_owner):
    tp_count = slice_owner.shape[0]
    dev_count = shard_block.shape[0]
    shard_rows = trainer_query.shape[1]
    features = trainer_query.shape[2]
    model_width = shard_rows * dev_count
    halves = 2
    width = halves * LANES
    probe_count = probes.shape[0]
    bf16, f32 = jnp.bfloat16, jnp.float32
    smem = pl.BlockSpec(memory_space=pltpu.SMEM)
    vmem = pl.BlockSpec(memory_space=pltpu.VMEM)
    hbm = pl.BlockSpec(memory_space=pltpu.HBM)

    packed = pl.pallas_call(
        pack_kernel,
        out_shape=jax.ShapeDtypeStruct((dev_count, shard_rows, width), bf16),
        in_specs=[hbm, hbm, hbm],
        out_specs=vmem,
        scratch_shapes=[
            pltpu.SMEM((tp_count,), jnp.int32),
            pltpu.VMEM((shard_rows, features), f32),
            pltpu.VMEM((shard_rows, features), f32),
            pltpu.SMEM((tp_count,), jnp.int32),
            pltpu.SemaphoreType.DMA((2, 8)),
            pltpu.SemaphoreType.DMA(()),
        ],
        compiler_params=params(12),
        name="pack",
    )(in_hbm(slice_owner), in_hbm(trainer_query[0]), in_hbm(trainer_output[0].T))

    recv = lax.all_to_all(packed, GROUP, split_axis=0, concat_axis=0, tiled=True)
    swap = [(0, 1), (1, 0)]
    other_recv = lax.ppermute(recv, "core", swap)

    prints, sent = pl.pallas_call(
        dot_kernel,
        out_shape=(
            jax.ShapeDtypeStruct((probe_count, width), f32),
            jax.ShapeDtypeStruct((probe_count, width), bf16),
        ),
        in_specs=[smem, vmem, vmem],
        out_specs=(vmem, vmem),
        scratch_shapes=[pltpu.VMEM((model_width, width), bf16), pltpu.SMEM((dev_count,), jnp.int32)],
        compiler_params=params(14),
        name="prints",
    )(shard_block, recv, probes)
    other_prints = lax.ppermute(sent, "core", swap)

    half = dict(
        out_shape=(
            jax.ShapeDtypeStruct((model_width, width), bf16),
            jax.ShapeDtypeStruct((width, model_width), bf16),
            jax.ShapeDtypeStruct((probe_count, width), f32),
            jax.ShapeDtypeStruct((width, probe_count), f32),
        ),
        out_specs=(hbm,) * 4,
        scratch_shapes=[
            pltpu.SMEM((dev_count,), jnp.int32),
            pltpu.VMEM((LANES, model_width), bf16),
            pltpu.VMEM((probe_count, LANES), f32),
            pltpu.VMEM((LANES, probe_count), f32),
            pltpu.SMEM((dev_count,), jnp.int32),
            pltpu.SemaphoreType.DMA((5,)),
        ],
        compiler_params=params(12),
    )
    outs = pl.pallas_call(own_kernel, in_specs=[vmem] * 3, name="own_half", **half)(shard_block, recv, prints)
    outs = pl.pallas_call(
        other_kernel,
        in_specs=[vmem] * 3 + [hbm] * 4,
        input_output_aliases={3: 0, 4: 1, 5: 2, 6: 3},
        name="other_half",
        **half,
    )(shard_block, other_recv, other_prints, *outs)
    return tuple(out[None] for out in outs)


def solution(mesh):
    fine = Mesh(mesh.devices.reshape(SIZES), AXES)
    placed = (P(AXES, None, None), P(AXES, None, None), P(), P(), P())
    out = P(("z", "xl", "y"), None, None)
    return jax.shard_map(per_device, mesh=fine, in_specs=placed, out_specs=(out, out, out, out), check_vma=False)
```
